32 devices in a mesh: dp: 8 (over z, y), owner: 4 (over x, core).
Axes of the slice: x: 2, y: 2, z: 4, core: 2. Of those that a mesh axis runs over, the one named last changes fastest.
Arguments:
- grads: float32 [8, 32, 512, 128], P('dp', None, 'owner'), may hold values from -21 to 21
- momentum: float32 [64, 512, 128], P('dp', 'owner'), may hold values from -30 to 30
- slot_matrix: int32 [64], replicated, may hold values from -1 to 31, as said below
Outputs:
- updates: bfloat16 [32, 512, 128], P(None, 'owner')
- momentum_out: float32 [64, 512, 128], P('dp', 'owner')
The draws below stay inside these ranges and needn't reach their ends.
Inputs may be any that keep to these rules, and one draw needn't show every extreme that they name: `slot_matrix`: entry s names the block held by slot s, or is -1 if slot s is empty; slots s with s // 8 == g belong to the owner group at index g of dp. Every one of the 32 blocks is held by exactly one slot, and some group, drawn from the seed, has all 8 slots filled.
All inputs are finite; a program needn't handle non-finite values.
Results may differ from the reference program's by a relative error of at most 0.038.
Values may be sent and summed in bfloat16 or wider, within the bound.
A program may use at most 64 MiB of HBM per device.

```python
import math
import jax
import jax.numpy as jnp
from jax import lax

C = 512
R = 128
SLOTS = 8
ITERS = 5
MATS = 32
TOTAL_SLOTS = 64
N_DP = 8


def shape_scales(key):
    key_cols, key_rows = jax.random.split(jax.random.fold_in(key, 11))
    columns = jnp.exp(jax.random.uniform(key_cols, (C,), jnp.float32, 0.0, math.log(10.0)))
    trend = 3.0 ** (jnp.arange(C, dtype=jnp.float32) / (C - 1))
    columns = columns * trend
    rows_scale = jnp.exp(jax.random.uniform(key_rows, (R,), jnp.float32, 0.0, math.log(10.0)))
    both = columns[:, None] * rows_scale[None, :]
    return both / jnp.max(both)


def draw_grads(key, part):
    scaled = shape_scales(key)
    key_rep = jax.random.fold_in(jax.random.fold_in(key, 23), 0)
    key_noise = jax.random.fold_in(jax.random.fold_in(key, 23), 2)
    replica = jnp.exp(jax.random.uniform(key_rep, (N_DP, MATS, 1, 1), jnp.float32, -1.2, 1.2))
    values = jnp.clip(jax.random.normal(key_noise, (N_DP, MATS, C, R), jnp.float32), -5.0, 5.0)
    return 6.0 * values * replica * scaled / math.sqrt(N_DP)


def draw_momentum(key, part):
    scaled = shape_scales(key)
    key_noise = jax.random.fold_in(key, 37)
    values = jnp.clip(jax.random.normal(key_noise, (TOTAL_SLOTS, C, R), jnp.float32), -5.0, 5.0)
    return 6.0 * values * scaled


def draw_slot_matrix(key, part):
    key_full, key_score, key_ids = jax.random.split(jax.random.fold_in(key, 53), 3)
    filled_group = jax.random.randint(key_full, (), 0, N_DP)
    positions = jnp.arange(TOTAL_SLOTS, dtype=jnp.int32)
    score = jax.random.permutation(key_score, TOTAL_SLOTS).astype(jnp.int32) + TOTAL_SLOTS
    score = jnp.where(positions // SLOTS == filled_group, positions % SLOTS, score)
    ordering = jnp.argsort(score, stable=True).astype(jnp.int32)
    identity = jax.random.permutation(key_ids, MATS).astype(jnp.int32)
    holder = jnp.full((TOTAL_SLOTS,), -1, jnp.int32)
    return holder.at[ordering[:MATS]].set(identity)


def setup_inputs(seed: int = 0) -> dict:
    splits = jax.random.split(jax.random.key(seed), 4)
    grads = draw_grads(jax.random.fold_in(splits[3], 71), 0)
    momentum = draw_momentum(jax.random.fold_in(splits[3], 71), 0)
    slot_matrix = draw_slot_matrix(jax.random.fold_in(splits[3], 71), 0)
    return dict(grads=grads, momentum=momentum, slot_matrix=slot_matrix)


momentum_rate = 0.95
epsilon_norm = 1e-07
first_coef = 3.4445
third_coef = -4.775
fifth_coef = 2.0315

def orthogonal(initial):
    iterate = initial
    advanced = initial.astype(jnp.float32)
    for iteration in range(ITERS):
        gram_matrix = jnp.dot(iterate.T, iterate, preferred_element_type=jnp.float32).astype(jnp.bfloat16)
        square = jnp.dot(gram_matrix, gram_matrix, preferred_element_type=jnp.float32)
        polynomial = (third_coef * gram_matrix.astype(jnp.float32) + fifth_coef * square).astype(jnp.bfloat16)
        advanced = first_coef * iterate.astype(jnp.float32) + jnp.dot(iterate, polynomial, preferred_element_type=jnp.float32)
        if iteration + 1 < ITERS:
            iterate = advanced.astype(jnp.bfloat16)
    return (math.sqrt(C) * advanced).astype(jnp.bfloat16)

def reference(grads, momentum, slot_matrix):
    summed = lax.optimization_barrier(jnp.sum(grads, axis=0))
    present = (slot_matrix >= 0).astype(jnp.float32)
    picked = jnp.take(summed, jnp.maximum(slot_matrix, 0).astype(jnp.int32), axis=0) * present[:, None, None]
    renewed = momentum_rate * momentum + picked
    norms = jnp.sqrt(lax.optimization_barrier(jnp.sum(renewed * renewed, axis=(1, 2))))
    initial = (renewed / (norms + epsilon_norm)[:, None, None]).astype(jnp.bfloat16)
    matches = slot_matrix[None, :] == jnp.arange(MATS, dtype=jnp.int32)[:, None]
    slot_of = lax.optimization_barrier(jnp.sum(jnp.where(matches, jnp.arange(TOTAL_SLOTS, dtype=jnp.int32)[None, :], 0), axis=1)).astype(jnp.int32)
    chosen = jnp.take(initial, slot_of, axis=0)
    updates = lax.map(orthogonal, chosen)
    return (updates, renewed)
```

```python
import functools
import math

import jax
import jax.numpy as jnp
from jax import lax
from jax.experimental import pallas as pl
from jax.experimental.pallas import tpu as pltpu
from jax.sharding import PartitionSpec as P

ITERS = 5

momentum_rate = 0.95
epsilon_norm = 1e-07
first_coef = 3.4445
third_coef = -4.775
fifth_coef = 2.0315

MESH = pl.DeviceIdType.MESH
F32 = jnp.float32
BF16 = jnp.bfloat16


def orthogonal(x):
    rows = x.shape[0]
    norm = jnp.sqrt(jnp.sum(x * x, axis=(0, 1), keepdims=True)) + epsilon_norm
    iterate = (x / norm).astype(BF16)
    advanced = None
    for iteration in range(ITERS):
        gram = lax.dot_general(
            iterate, iterate, (((0,), (0,)), ((), ())), preferred_element_type=F32
        ).astype(BF16)
        square = jnp.dot(gram, gram, preferred_element_type=F32)
        poly = (third_coef * gram.astype(F32) + fifth_coef * square).astype(BF16)
        advanced = first_coef * iterate.astype(F32) + jnp.dot(
            iterate, poly, preferred_element_type=F32
        )
        iterate = advanced.astype(BF16)
    return (math.sqrt(rows) * advanced).astype(BF16)


def kernel(
    n_dp, n_ow, per, workers,
    slots_ref, grads_ref, mom_ref, upd_ref, momout_ref,
    ypack, yrecv, zsend, zrecv, own, held, orecv, ubuf, every, ysel, yselrecv,
    ys, yr, zs, zr, os_, or_, ms, mr, qs, qr, us, ur, vs, vr, ws, wr,
):
    n_z = n_dp // 2
    mats = grads_ref.shape[0]
    nb = mats // n_dp
    n_slots = mom_ref.shape[0]
    dp = lax.axis_index("dp")
    ow = lax.axis_index("owner")
    z = lax.div(dp, 2)
    y = lax.rem(dp, 2)
    other = 2 * z + 1 - y

    def up(t):
        return lax.rem(z + 1 + t, n_z)

    def down(t):
        return lax.rem(z - 1 - t + 2 * n_z, n_z)

    def owner_at(t):
        return lax.rem(ow + t, n_ow)

    def owner_from(t):
        return lax.rem(ow - t + n_ow, n_ow)

    def remote(src, dst, send, recv, to):
        return pltpu.make_async_remote_copy(
            src_ref=src, dst_ref=dst, send_sem=send, recv_sem=recv,
            device_id=to, device_id_type=MESH,
        )

    barrier = pltpu.get_barrier_semaphore()
    pl.semaphore_signal(barrier, inc=1, device_id=(other, ow), device_id_type=MESH)
    for t in range(n_z - 1):
        pl.semaphore_signal(barrier, inc=1, device_id=(2 * up(t) + y, ow), device_id_type=MESH)
    for t in range(1, n_ow):
        pl.semaphore_signal(barrier, inc=1, device_id=(dp, owner_at(t)), device_id_type=MESH)

    held_slots = [slots_ref[dp * n_slots + k] for k in range(n_slots)]

    def partial(m):
        place = jnp.int32(0)
        weight = F32(0.0)
        for k in range(n_slots):
            hit = held_slots[k] == m
            place = jnp.where(hit, k, place)
            weight = jnp.where(hit, F32(momentum_rate), weight)
        return grads_ref[m] + weight * mom_ref[place]

    y_copies = []
    for t in range(n_z):
        def pack(j, carry, t=t):
            ypack[t, j] = partial((2 * up(t) + 1 - y) * nb + j).astype(BF16)
            return carry
        lax.fori_loop(0, nb, pack, 0)
        if t == 0:
            pl.semaphore_wait(barrier, 1 + (n_z - 1) + (n_ow - 1))
        copy = remote(ypack.at[t], yrecv.at[t], ys.at[t], yr.at[t], (other, ow))
        copy.start()
        y_copies.append(copy)

    z_copies = []
    for t in range(n_z):
        y_copies[t].wait_recv()
        def add(j, carry, t=t):
            value = partial((2 * up(t) + y) * nb + j) + yrecv[t, j].astype(F32)
            if t < n_z - 1:
                zsend[t, j] = value.astype(BF16)
            else:
                own[j] = value
            return carry
        lax.fori_loop(0, nb, add, 0)
        if t < n_z - 1:
            copy = remote(zsend.at[t], zrecv.at[t], zs.at[t], zr.at[t], (2 * up(t) + y, ow))
            copy.start()
            z_copies.append(copy)

    for copy in z_copies:
        copy.wait_recv()

    mine = pl.ds(z * nb, nb)

    def total(j, carry):
        value = own[j]
        for t in range(n_z - 1):
            value = value + zrecv[t, j].astype(F32)
        held[z * nb + j] = value.astype(BF16)
        return carry
    lax.fori_loop(0, nb, total, 0)

    def when_worker(index, fn):
        if workers == n_ow:
            fn()
        else:
            pl.when(index < workers)(fn)

    def share(j):
        return pl.ds(j * per, per)

    o_copies = []
    for t in range(1, n_ow):
        j = owner_at(t)
        copy = remote(
            held.at[pl.ds(z * nb + j * per, per)], orecv.at[ow],
            os_.at[t - 1], or_.at[t - 1], (dp, j),
        )
        when_worker(j, copy.start)
        o_copies.append(copy)
    m_copies = []
    for t in range(n_z - 1):
        copy = remote(held.at[mine], held.at[mine], ms.at[t], mr.at[t], (2 * up(t) + y, ow))
        copy.start()
        m_copies.append(copy)

    def keep_own():
        orecv[ow] = held[pl.ds(z * nb + ow * per, per)]
    when_worker(ow, keep_own)

    def work():
        for copy in o_copies:
            copy.wait_recv()
        for p in range(per):
            pieces = [orecv[o, p].astype(F32) for o in range(n_ow)]
            update = orthogonal(jnp.concatenate(pieces, axis=0))
            rows = update.shape[0] // n_ow
            for o in range(n_ow):
                ubuf[o, p] = update[o * rows:(o + 1) * rows]
    when_worker(ow, work)

    home = pl.ds(dp * nb + ow * per, per)
    u_copies = []
    for t in range(1, n_ow):
        j = owner_at(t)
        copy = remote(ubuf.at[j], every.at[home], us.at[t - 1], ur.at[t - 1], (dp, j))
        when_worker(ow, copy.start)
        u_copies.append(copy)

    def keep_update():
        every[home] = ubuf[ow]
    when_worker(ow, keep_update)

    for copy in m_copies:
        copy.wait_recv()

    def place_of(m):
        m = jnp.maximum(m, 0)
        return lax.div(m, 2 * nb) * nb + lax.rem(m, nb)

    def pick(k, carry):
        ysel[k] = held[place_of(slots_ref[other * n_slots + k])]
        return carry
    lax.fori_loop(0, n_slots, pick, 0)
    q_copy = remote(ysel, yselrecv, qs, qr, (other, ow))
    q_copy.start()

    for t in range(1, n_ow):
        when_worker(owner_from(t), u_copies[t - 1].wait_recv)

    def chunk(g):
        return pl.ds(g * nb, nb)

    v_copies = []
    for t in range(n_z - 1):
        copy = remote(
            every.at[chunk(dp)], every.at[chunk(dp)], vs.at[t], vr.at[t], (2 * up(t) + y, ow)
        )
        copy.start()
        v_copies.append(copy)
    w_copies = []
    copy = remote(
        every.at[chunk(dp)], every.at[chunk(dp)], ws.at[n_z - 1], wr.at[n_z - 1], (other, ow)
    )
    copy.start()
    w_copies.append(copy)
    for t in range(n_z - 1):
        v_copies[t].wait_recv()
        g = 2 * down(t) + y
        copy = remote(every.at[chunk(g)], every.at[chunk(g)], ws.at[t], wr.at[t], (other, ow))
        copy.start()
        w_copies.append(copy)

    q_copy.wait_recv()

    def renew(k, carry):
        m = slots_ref[dp * n_slots + k]
        side = lax.rem(lax.div(jnp.maximum(m, 0), nb), 2)
        local = jnp.where(side == y, F32(1.0), F32(0.0))
        present = jnp.where(m >= 0, F32(1.0), F32(0.0))
        near = held[place_of(m)].astype(F32)
        far = yselrecv[k].astype(F32)
        summed = present * (local * near + (1.0 - local) * far)
        momout_ref[k] = summed + (1.0 - present) * (F32(momentum_rate) * mom_ref[k])
        return carry
    lax.fori_loop(0, n_slots, renew, 0)

    for copy in w_copies:
        copy.wait_recv()
    upd_ref[...] = every[...]

    for copy in y_copies + z_copies + m_copies + [q_copy] + v_copies + w_copies:
        copy.wait_send()
    for t in range(1, n_ow):
        when_worker(owner_at(t), o_copies[t - 1].wait_send)
        when_worker(ow, u_copies[t - 1].wait_send)


def local(n_dp, n_ow, grads, momentum, slot_matrix):
    mats, rows, cols = grads.shape[1:]
    n_slots = momentum.shape[0]
    nb = mats // n_dp
    n_z = n_dp // 2
    workers = min(nb, n_ow)
    per = nb // workers
    block = (rows, cols)
    vmem = pl.BlockSpec(memory_space=pltpu.VMEM)
    dma = pltpu.SemaphoreType.DMA
    counts = (n_z, n_z - 1, n_ow - 1, n_z - 1, None, n_ow - 1, n_z - 1, n_z)
    sems = []
    for count in counts:
        sems += [dma if count is None else dma((count,))] * 2
    updates, renewed = pl.pallas_call(
        functools.partial(kernel, n_dp, n_ow, per, workers),
        out_shape=(
            jax.ShapeDtypeStruct((mats,) + block, BF16),
            jax.ShapeDtypeStruct(momentum.shape, F32),
        ),
        in_specs=[pl.BlockSpec(memory_space=pltpu.SMEM), vmem, vmem],
        out_specs=(vmem, vmem),
        scratch_shapes=[
            pltpu.VMEM((n_z, nb) + block, BF16),
            pltpu.VMEM((n_z, nb) + block, BF16),
            pltpu.VMEM((n_z - 1, nb) + block, BF16),
            pltpu.VMEM((n_z - 1, nb) + block, BF16),
            pltpu.VMEM((nb,) + block, F32),
            pltpu.VMEM((n_z * nb,) + block, BF16),
            pltpu.VMEM((n_ow, per) + block, BF16),
            pltpu.VMEM((n_ow, per) + block, BF16),
            pltpu.VMEM((mats,) + block, BF16),
            pltpu.VMEM((n_slots,) + block, BF16),
            pltpu.VMEM((n_slots,) + block, BF16),
        ] + sems,
        compiler_params=pltpu.CompilerParams(collective_id=0, has_side_effects=True),
    )(slot_matrix, grads[0], momentum)
    return updates, renewed


def solution(mesh):
    return jax.shard_map(
        functools.partial(local, mesh.shape["dp"], mesh.shape["owner"]),
        mesh=mesh,
        in_specs=(P("dp", None, "owner", None), P("dp", "owner", None), P()),
        out_specs=(P(None, "owner", None), P("dp", "owner", None)),
        check_vma=False,
    )
```

```python
import functools
import math

import jax
import jax.numpy as jnp
from jax import lax
from jax.experimental import pallas as pl
from jax.experimental.pallas import tpu as pltpu
from jax.sharding import PartitionSpec as P

ITERS = 5

momentum_rate = 0.95
epsilon_norm = 1e-07
first_coef = 3.4445
third_coef = -4.775
fifth_coef = 2.0315

MESH = pl.DeviceIdType.MESH
F32 = jnp.float32
BF16 = jnp.bfloat16


def normalized(x):
    norm = jnp.sqrt(jnp.sum(x * x, axis=(0, 1), keepdims=True)) + epsilon_norm
    return (x / norm).astype(BF16)


def sweep(iterate):
    gram = lax.dot_general(
        iterate, iterate, (((0,), (0,)), ((), ())), preferred_element_type=F32
    ).astype(BF16)
    square = jnp.dot(gram, gram, preferred_element_type=F32)
    poly = (third_coef * gram.astype(F32) + fifth_coef * square).astype(BF16)
    return first_coef * iterate.astype(F32) + jnp.dot(iterate, poly, preferred_element_type=F32)


def kernel(
    n_dp, n_ow, per, workers,
    slots_ref, grads_ref, mom_ref, upd_ref, momout_ref,
    ypack, yrecv, zsend, zrecv, own, held, orecv, work, ubuf, every, ysel, yselrecv,
    ys, yr, zs, zr, os_, or_, ms, mr, qs, qr, us, ur, vs, vr, ws, wr, bs, br,
):
    n_z = n_dp // 2
    mats = grads_ref.shape[0]
    nb = mats // n_dp
    n_slots = mom_ref.shape[0]
    dp = lax.axis_index("dp")
    ow = lax.axis_index("owner")
    z = lax.div(dp, 2)
    y = lax.rem(dp, 2)
    other = 2 * z + 1 - y

    def up(t):
        return lax.rem(z + 1 + t, n_z)

    def down(t):
        return lax.rem(z - 1 - t + 2 * n_z, n_z)

    def owner_at(t):
        return lax.rem(ow + t, n_ow)

    def owner_from(t):
        return lax.rem(ow - t + n_ow, n_ow)

    def remote(src, dst, send, recv, to):
        return pltpu.make_async_remote_copy(
            src_ref=src, dst_ref=dst, send_sem=send, recv_sem=recv,
            device_id=to, device_id_type=MESH,
        )

    barrier = pltpu.get_barrier_semaphore()
    pl.semaphore_signal(barrier, inc=1, device_id=(other, ow), device_id_type=MESH)
    for t in range(n_z - 1):
        pl.semaphore_signal(barrier, inc=1, device_id=(2 * up(t) + y, ow), device_id_type=MESH)
    for t in range(1, n_ow):
        pl.semaphore_signal(barrier, inc=1, device_id=(dp, owner_at(t)), device_id_type=MESH)

    held_slots = [slots_ref[dp * n_slots + k] for k in range(n_slots)]

    def partial(m):
        place = jnp.int32(0)
        weight = F32(0.0)
        for k in range(n_slots):
            hit = held_slots[k] == m
            place = jnp.where(hit, k, place)
            weight = jnp.where(hit, F32(momentum_rate), weight)
        return grads_ref[m] + weight * mom_ref[place]

    y_copies = []
    for t in range(n_z):
        def pack(j, carry, t=t):
            ypack[t, j] = partial((2 * up(t) + 1 - y) * nb + j).astype(BF16)
            return carry
        lax.fori_loop(0, nb, pack, 0)
        if t == 0:
            pl.semaphore_wait(barrier, 1 + (n_z - 1) + (n_ow - 1))
        copy = remote(ypack.at[t], yrecv.at[t], ys.at[t], yr.at[t], (other, ow))
        copy.start()
        y_copies.append(copy)

    z_copies = []
    for t in range(n_z):
        y_copies[t].wait_recv()
        def add(j, carry, t=t):
            value = partial((2 * up(t) + y) * nb + j) + yrecv[t, j].astype(F32)
            if t < n_z - 1:
                zsend[t, j] = value.astype(BF16)
            else:
                own[j] = value
            return carry
        lax.fori_loop(0, nb, add, 0)
        if t < n_z - 1:
            copy = remote(zsend.at[t], zrecv.at[t], zs.at[t], zr.at[t], (2 * up(t) + y, ow))
            copy.start()
            z_copies.append(copy)

    for copy in z_copies:
        copy.wait_recv()

    mine = pl.ds(z * nb, nb)

    def total(j, carry):
        value = own[j]
        for t in range(n_z - 1):
            value = value + zrecv[t, j].astype(F32)
        held[z * nb + j] = value.astype(BF16)
        return carry
    lax.fori_loop(0, nb, total, 0)

    def when_worker(index, fn):
        if workers == n_ow:
            fn()
        else:
            pl.when(index < workers)(fn)

    def share(j):
        return pl.ds(j * per, per)

    o_copies = []
    for t in range(1, n_ow):
        j = owner_at(t)
        copy = remote(
            held.at[pl.ds(z * nb + j * per, per)], orecv.at[ow],
            os_.at[t - 1], or_.at[t - 1], (dp, j),
        )
        when_worker(j, copy.start)
        o_copies.append(copy)
    flows = ((1, z < n_z - 1), (-1, z > 0))

    def within(index):
        return jnp.logical_and(index >= 0, index < n_z)

    def leg(f, k, item, region, buf, send, recv):
        step, open_ahead = flows[f]
        chunk = z - step * k
        where = region(chunk)
        to = jnp.clip(z + step, 0, n_z - 1)
        copy = remote(
            buf.at[where], buf.at[where], send.at[f, k, item], recv.at[f, k, item],
            (2 * to + y, ow),
        )
        sends = jnp.logical_and(open_ahead, within(chunk))
        takes = within(chunk - step)
        return copy, sends, takes

    pending = []

    def launch(legs, k, item):
        for f in range(2):
            copy, sends, _ = legs(f, k, item)
            pl.when(sends)(copy.start)
            pending.append((copy, sends))

    def arrive(legs, k, item):
        for f in range(2):
            copy, _, takes = legs(f, k, item)
            pl.when(takes)(copy.wait_recv)

    half = nb // 2
    parts = ((0, half), (half, nb - half))

    def m_legs(f, k, item):
        first, count = parts[item]
        return leg(f, k, item, lambda c: pl.ds(c * nb + first, count), held, ms, mr)

    def m_pass(k, item):
        if k > 0:
            arrive(m_legs, k - 1, item)
        if k < n_z - 1:
            launch(m_legs, k, item)

    m_pass(0, 0)
    m_pass(0, 1)

    def keep_own():
        orecv[ow] = held[pl.ds(z * nb + ow * per, per)]
    when_worker(ow, keep_own)

    def begin():
        for copy in o_copies:
            copy.wait_recv()
        for p in range(per):
            pieces = [orecv[o, p].astype(F32) for o in range(n_ow)]
            work[p] = normalized(jnp.concatenate(pieces, axis=0))

    def sweeps(count):
        def run():
            for p in range(per):
                iterate = work[p]
                for _ in range(count):
                    iterate = sweep(iterate).astype(BF16)
                work[p] = iterate
        return run

    def end():
        for p in range(per):
            advanced = sweep(work[p])
            update = (math.sqrt(advanced.shape[0]) * advanced).astype(BF16)
            rows = update.shape[0] // n_ow
            for o in range(n_ow):
                ubuf[o, p] = update[o * rows:(o + 1) * rows]

    before = (ITERS - 1) // 2
    when_worker(ow, begin)
    m_pass(1, 0)
    when_worker(ow, sweeps(before))
    m_pass(1, 1)
    when_worker(ow, sweeps(ITERS - 1 - before))
    when_worker(ow, end)

    home = pl.ds(dp * nb + ow * per, per)
    u_copies = []
    for t in range(1, n_ow):
        j = owner_at(t)
        copy = remote(ubuf.at[j], every.at[home], us.at[t - 1], ur.at[t - 1], (dp, j))
        when_worker(ow, copy.start)
        u_copies.append(copy)

    def keep_update():
        every[home] = ubuf[ow]
    when_worker(ow, keep_update)

    for k in range(2, n_z - 1):
        for item in range(2):
            m_pass(k, item)

    for t in range(1, n_ow):
        when_worker(owner_from(t), u_copies[t - 1].wait_recv)

    def v_region(item):
        first, count = parts[0] if item == 0 else parts[1]
        side = 1 - y if item == 2 else y
        return lambda c: pl.ds((2 * c + side) * nb + first, count)

    def v_legs(f, k, item):
        return leg(f, k, item, v_region(item), every, vs, vr)

    b_own = every.at[v_region(1)(z)]
    b_copy = remote(b_own, b_own, bs, br, (other, ow))
    b_copy.start()
    launch(v_legs, 0, 0)
    launch(v_legs, 0, 1)

    def across(chunk, sem):
        piece = every.at[v_region(0)(chunk)]
        return remote(piece, piece, ws.at[sem], wr.at[sem], (other, ow))

    a_copies = [(across(z, 2 * (n_z - 1)), None)]
    a_copies[0][0].start()

    m_pass(n_z - 1, 0)
    m_pass(n_z - 1, 1)

    def place_of(m):
        m = jnp.maximum(m, 0)
        return lax.div(m, 2 * nb) * nb + lax.rem(m, nb)

    def pick(k, carry):
        ysel[k] = held[place_of(slots_ref[other * n_slots + k])]
        return carry
    lax.fori_loop(0, n_slots, pick, 0)
    q_copy = remote(ysel, yselrecv, qs, qr, (other, ow))
    q_copy.start()

    b_copy.wait_recv()
    launch(v_legs, 0, 2)

    def v_pass(k):
        for item in range(3):
            arrive(v_legs, k - 1, item)
            if k < n_z - 1:
                launch(v_legs, k, item)
            if item == 0:
                for f in range(2):
                    chunk = z - flows[f][0] * k
                    copy = across(chunk, 2 * (k - 1) + f)
                    pl.when(within(chunk))(copy.start)
                    a_copies.append((copy, within(chunk)))

    for k in range(1, n_z - 1):
        v_pass(k)

    q_copy.wait_recv()

    def renew(k, carry):
        m = slots_ref[dp * n_slots + k]
        side = lax.rem(lax.div(jnp.maximum(m, 0), nb), 2)
        local = jnp.where(side == y, F32(1.0), F32(0.0))
        present = jnp.where(m >= 0, F32(1.0), F32(0.0))
        near = held[place_of(m)].astype(F32)
        far = yselrecv[k].astype(F32)
        summed = present * (local * near + (1.0 - local) * far)
        momout_ref[k] = summed + (1.0 - present) * (F32(momentum_rate) * mom_ref[k])
        return carry
    lax.fori_loop(0, n_slots, renew, 0)

    v_pass(n_z - 1)
    for copy, there in a_copies:
        if there is None:
            copy.wait_recv()
        else:
            pl.when(there)(copy.wait_recv)
    upd_ref[...] = every[...]

    for copy in y_copies + z_copies + [q_copy, b_copy, a_copies[0][0]]:
        copy.wait_send()
    for copy, sent in pending + a_copies[1:]:
        pl.when(sent)(copy.wait_send)
    for t in range(1, n_ow):
        when_worker(owner_at(t), o_copies[t - 1].wait_send)
        when_worker(ow, u_copies[t - 1].wait_send)


def local(n_dp, n_ow, grads, momentum, slot_matrix):
    mats, rows, cols = grads.shape[1:]
    n_slots = momentum.shape[0]
    nb = mats // n_dp
    n_z = n_dp // 2
    workers = min(nb, n_ow)
    per = nb // workers
    block = (rows, cols)
    vmem = pl.BlockSpec(memory_space=pltpu.VMEM)
    dma = pltpu.SemaphoreType.DMA
    hops = n_z - 1
    counts = (
        (n_z,), (hops,), (n_ow - 1,), (2, hops, 2), (), (n_ow - 1,), (2, hops, 3), (2 * hops + 1,), ()
    )
    sems = []
    for count in counts:
        sems += [dma(count) if count else dma] * 2
    updates, renewed = pl.pallas_call(
        functools.partial(kernel, n_dp, n_ow, per, workers),
        out_shape=(
            jax.ShapeDtypeStruct((mats,) + block, BF16),
            jax.ShapeDtypeStruct(momentum.shape, F32),
        ),
        in_specs=[pl.BlockSpec(memory_space=pltpu.SMEM), vmem, vmem],
        out_specs=(vmem, vmem),
        scratch_shapes=[
            pltpu.VMEM((n_z, nb) + block, BF16),
            pltpu.VMEM((n_z, nb) + block, BF16),
            pltpu.VMEM((n_z - 1, nb) + block, BF16),
            pltpu.VMEM((n_z - 1, nb) + block, BF16),
            pltpu.VMEM((nb,) + block, F32),
            pltpu.VMEM((n_z * nb,) + block, BF16),
            pltpu.VMEM((n_ow, per) + block, BF16),
            pltpu.VMEM((per, n_ow * rows, cols), BF16),
            pltpu.VMEM((n_ow, per) + block, BF16),
            pltpu.VMEM((mats,) + block, BF16),
            pltpu.VMEM((n_slots,) + block, BF16),
            pltpu.VMEM((n_slots,) + block, BF16),
        ] + sems,
        compiler_params=pltpu.CompilerParams(collective_id=0, has_side_effects=True),
    )(slot_matrix, grads[0], momentum)
    return updates, renewed


def solution(mesh):
    return jax.shard_map(
        functools.partial(local, mesh.shape["dp"], mesh.shape["owner"]),
        mesh=mesh,
        in_specs=(P("dp", None, "owner", None), P("dp", "owner", None), P()),
        out_specs=(P(None, "owner", None), P("dp", "owner", None)),
        check_vma=False,
    )
```

```python
import functools
import math

import jax
import jax.numpy as jnp
from jax import lax
from jax.experimental import pallas as pl
from jax.experimental.pallas import tpu as pltpu
from jax.sharding import PartitionSpec as P

ITERS = 5

momentum_rate = 0.95
epsilon_norm = 1e-07
first_coef = 3.4445
third_coef = -4.775
fifth_coef = 2.0315

MESH = pl.DeviceIdType.MESH
F32 = jnp.float32
BF16 = jnp.bfloat16


def normalized(x):
    norm = jnp.sqrt(jnp.sum(x * x, axis=(0, 1), keepdims=True)) + epsilon_norm
    return (x / norm).astype(BF16)


def sweep(iterate):
    gram = lax.dot_general(
        iterate, iterate, (((0,), (0,)), ((), ())), preferred_element_type=F32
    ).astype(BF16)
    square = jnp.dot(gram, gram, preferred_element_type=F32)
    poly = (third_coef * gram.astype(F32) + fifth_coef * square).astype(BF16)
    return first_coef * iterate.astype(F32) + jnp.dot(iterate, poly, preferred_element_type=F32)


def kernel(
    n_dp, n_ow, per, workers,
    slots_ref, grads_ref, mom_ref, upd_ref, momout_ref,
    ypack, yrecv, zsend, zrecv, own, held, orecv, work, ubuf, every, ysel, yselrecv,
    ys, yr, zs, zr, os_, or_, ms, mr, qs, qr, us, ur, vs, vr, ws, wr, bs, br,
):
    n_z = n_dp // 2
    mats = grads_ref.shape[0]
    nb = mats // n_dp
    n_slots = mom_ref.shape[0]
    dp = lax.axis_index("dp")
    ow = lax.axis_index("owner")
    z = lax.div(dp, 2)
    y = lax.rem(dp, 2)
    other = 2 * z + 1 - y

    def up(t):
        return lax.rem(z + 1 + t, n_z)

    def down(t):
        return lax.rem(z - 1 - t + 2 * n_z, n_z)

    def owner_at(t):
        return lax.rem(ow + t, n_ow)

    def owner_from(t):
        return lax.rem(ow - t + n_ow, n_ow)

    def remote(src, dst, send, recv, to):
        return pltpu.make_async_remote_copy(
            src_ref=src, dst_ref=dst, send_sem=send, recv_sem=recv,
            device_id=to, device_id_type=MESH,
        )

    barrier = pltpu.get_barrier_semaphore()
    pl.semaphore_signal(barrier, inc=1, device_id=(other, ow), device_id_type=MESH)
    for t in range(n_z - 1):
        pl.semaphore_signal(barrier, inc=1, device_id=(2 * up(t) + y, ow), device_id_type=MESH)
    for t in range(1, n_ow):
        pl.semaphore_signal(barrier, inc=1, device_id=(dp, owner_at(t)), device_id_type=MESH)

    held_slots = [slots_ref[dp * n_slots + k] for k in range(n_slots)]

    def partial(m):
        place = jnp.int32(0)
        weight = F32(0.0)
        for k in range(n_slots):
            hit = held_slots[k] == m
            place = jnp.where(hit, k, place)
            weight = jnp.where(hit, F32(momentum_rate), weight)
        return grads_ref[m] + weight * mom_ref[place]

    y_copies = []
    for t in range(n_z):
        def pack(j, carry, t=t):
            ypack[t, j] = partial((2 * up(t) + 1 - y) * nb + j).astype(BF16)
            return carry
        lax.fori_loop(0, nb, pack, 0)
        if t == 0:
            pl.semaphore_wait(barrier, 1 + (n_z - 1) + (n_ow - 1))
        copy = remote(ypack.at[t], yrecv.at[t], ys.at[t], yr.at[t], (other, ow))
        copy.start()
        y_copies.append(copy)

    z_copies = []
    for t in range(n_z):
        y_copies[t].wait_recv()
        def add(j, carry, t=t):
            value = partial((2 * up(t) + y) * nb + j) + yrecv[t, j].astype(F32)
            if t < n_z - 1:
                zsend[t, j] = value.astype(BF16)
            else:
                own[j] = value
            return carry
        lax.fori_loop(0, nb, add, 0)
        if t < n_z - 1:
            copy = remote(zsend.at[t], zrecv.at[t], zs.at[t], zr.at[t], (2 * up(t) + y, ow))
            copy.start()
            z_copies.append(copy)

    for copy in z_copies:
        copy.wait_recv()

    mine = pl.ds(z * nb, nb)

    def total(j, carry):
        value = own[j]
        for t in range(n_z - 1):
            value = value + zrecv[t, j].astype(F32)
        held[z * nb + j] = value.astype(BF16)
        return carry
    lax.fori_loop(0, nb, total, 0)

    def when_worker(index, fn):
        if workers == n_ow:
            fn()
        else:
            pl.when(index < workers)(fn)

    def share(j):
        return pl.ds(j * per, per)

    o_copies = []
    for t in range(1, n_ow):
        j = owner_at(t)
        copy = remote(
            held.at[pl.ds(z * nb + j * per, per)], orecv.at[ow],
            os_.at[t - 1], or_.at[t - 1], (dp, j),
        )
        when_worker(j, copy.start)
        o_copies.append(copy)
    flows = ((1, z < n_z - 1), (-1, z > 0))

    def within(index):
        return jnp.logical_and(index >= 0, index < n_z)

    def leg(f, k, item, region, buf, send, recv):
        step, open_ahead = flows[f]
        chunk = z - step * k
        where = region(chunk)
        to = jnp.clip(z + step, 0, n_z - 1)
        copy = remote(
            buf.at[where], buf.at[where], send.at[f, k, item], recv.at[f, k, item],
            (2 * to + y, ow),
        )
        sends = jnp.logical_and(open_ahead, within(chunk))
        takes = within(chunk - step)
        return copy, sends, takes

    pending = []

    def launch(legs, k, item):
        for f in range(2):
            copy, sends, _ = legs(f, k, item)
            pl.when(sends)(copy.start)
            pending.append((copy, sends))

    def arrive(legs, k, item):
        for f in range(2):
            copy, _, takes = legs(f, k, item)
            pl.when(takes)(copy.wait_recv)

    half = nb // 2
    parts = ((0, half), (half, nb - half))

    def m_legs(f, k, item):
        first, count = parts[item]
        return leg(f, k, item, lambda c: pl.ds(c * nb + first, count), held, ms, mr)

    def m_pass(k, item):
        if k > 0:
            arrive(m_legs, k - 1, item)
        if k < n_z - 1:
            launch(m_legs, k, item)

    m_pass(0, 0)
    m_pass(0, 1)

    def keep_own():
        orecv[ow] = held[pl.ds(z * nb + ow * per, per)]
    when_worker(ow, keep_own)

    def begin():
        for copy in o_copies:
            copy.wait_recv()
        for p in range(per):
            pieces = [orecv[o, p].astype(F32) for o in range(n_ow)]
            work[p] = normalized(jnp.concatenate(pieces, axis=0))

    def sweeps(count):
        def run():
            for p in range(per):
                iterate = work[p]
                for _ in range(count):
                    iterate = sweep(iterate).astype(BF16)
                work[p] = iterate
        return run

    def end():
        for p in range(per):
            advanced = sweep(work[p])
            update = (math.sqrt(advanced.shape[0]) * advanced).astype(BF16)
            rows = update.shape[0] // n_ow
            for o in range(n_ow):
                ubuf[o, p] = update[o * rows:(o + 1) * rows]

    before = (ITERS - 1) // 2
    when_worker(ow, begin)
    m_pass(1, 0)
    when_worker(ow, sweeps(before))
    m_pass(1, 1)
    when_worker(ow, sweeps(ITERS - 1 - before))
    when_worker(ow, end)

    home = pl.ds(dp * nb + ow * per, per)
    u_copies = []
    for t in range(1, n_ow):
        j = owner_at(t)
        copy = remote(ubuf.at[j], every.at[home], us.at[t - 1], ur.at[t - 1], (dp, j))
        when_worker(ow, copy.start)
        u_copies.append(copy)

    def keep_update():
        every[home] = ubuf[ow]
    when_worker(ow, keep_update)

    for k in range(2, n_z - 1):
        for item in range(2):
            m_pass(k, item)

    for t in range(1, n_ow):
        when_worker(owner_from(t), u_copies[t - 1].wait_recv)

    def v_region(item):
        first, count = parts[0] if item == 0 else parts[1]
        side = 1 - y if item == 2 else y
        return lambda c: pl.ds((2 * c + side) * nb + first, count)

    def v_legs(f, k, item):
        return leg(f, k, item, v_region(item), every, vs, vr)

    b_own = every.at[v_region(1)(z)]
    b_copy = remote(b_own, b_own, bs, br, (other, ow))
    b_copy.start()
    launch(v_legs, 0, 0)
    launch(v_legs, 0, 1)

    def across(chunk, sem):
        piece = every.at[v_region(0)(chunk)]
        return remote(piece, piece, ws.at[sem], wr.at[sem], (other, ow))

    a_copies = [(across(z, 2 * (n_z - 1)), None)]
    a_copies[0][0].start()

    b_copy.wait_recv()
    launch(v_legs, 0, 2)

    m_pass(n_z - 1, 0)
    m_pass(n_z - 1, 1)

    def place_of(m):
        m = jnp.maximum(m, 0)
        return lax.div(m, 2 * nb) * nb + lax.rem(m, nb)

    def pick(k, carry):
        ysel[k] = held[place_of(slots_ref[other * n_slots + k])]
        return carry
    lax.fori_loop(0, n_slots, pick, 0)
    q_copy = remote(ysel, yselrecv, qs, qr, (other, ow))
    q_copy.start()


    def v_pass(k):
        for item in range(3):
            arrive(v_legs, k - 1, item)
            if k < n_z - 1:
                launch(v_legs, k, item)
            if item == 0:
                for f in range(2):
                    chunk = z - flows[f][0] * k
                    copy = across(chunk, 2 * (k - 1) + f)
                    pl.when(within(chunk))(copy.start)
                    a_copies.append((copy, within(chunk)))

    for k in range(1, n_z - 1):
        v_pass(k)

    q_copy.wait_recv()

    def renew(k, carry):
        m = slots_ref[dp * n_slots + k]
        side = lax.rem(lax.div(jnp.maximum(m, 0), nb), 2)
        local = jnp.where(side == y, F32(1.0), F32(0.0))
        present = jnp.where(m >= 0, F32(1.0), F32(0.0))
        near = held[place_of(m)].astype(F32)
        far = yselrecv[k].astype(F32)
        summed = present * (local * near + (1.0 - local) * far)
        momout_ref[k] = summed + (1.0 - present) * (F32(momentum_rate) * mom_ref[k])
        return carry
    lax.fori_loop(0, n_slots, renew, 0)

    v_pass(n_z - 1)
    for copy, there in a_copies:
        if there is None:
            copy.wait_recv()
        else:
            pl.when(there)(copy.wait_recv)
    upd_ref[...] = every[...]

    for copy in y_copies + z_copies + [q_copy, b_copy, a_copies[0][0]]:
        copy.wait_send()
    for copy, sent in pending + a_copies[1:]:
        pl.when(sent)(copy.wait_send)
    for t in range(1, n_ow):
        when_worker(owner_at(t), o_copies[t - 1].wait_send)
        when_worker(ow, u_copies[t - 1].wait_send)


def local(n_dp, n_ow, grads, momentum, slot_matrix):
    mats, rows, cols = grads.shape[1:]
    n_slots = momentum.shape[0]
    nb = mats // n_dp
    n_z = n_dp // 2
    workers = min(nb, n_ow)
    per = nb // workers
    block = (rows, cols)
    vmem = pl.BlockSpec(memory_space=pltpu.VMEM)
    dma = pltpu.SemaphoreType.DMA
    hops = n_z - 1
    counts = (
        (n_z,), (hops,), (n_ow - 1,), (2, hops, 2), (), (n_ow - 1,), (2, hops, 3), (2 * hops + 1,), ()
    )
    sems = []
    for count in counts:
        sems += [dma(count) if count else dma] * 2
    updates, renewed = pl.pallas_call(
        functools.partial(kernel, n_dp, n_ow, per, workers),
        out_shape=(
            jax.ShapeDtypeStruct((mats,) + block, BF16),
            jax.ShapeDtypeStruct(momentum.shape, F32),
        ),
        in_specs=[pl.BlockSpec(memory_space=pltpu.SMEM), vmem, vmem],
        out_specs=(vmem, vmem),
        scratch_shapes=[
            pltpu.VMEM((n_z, nb) + block, BF16),
            pltpu.VMEM((n_z, nb) + block, BF16),
            pltpu.VMEM((n_z - 1, nb) + block, BF16),
            pltpu.VMEM((n_z - 1, nb) + block, BF16),
            pltpu.VMEM((nb,) + block, F32),
            pltpu.VMEM((n_z * nb,) + block, BF16),
            pltpu.VMEM((n_ow, per) + block, BF16),
            pltpu.VMEM((per, n_ow * rows, cols), BF16),
            pltpu.VMEM((n_ow, per) + block, BF16),
            pltpu.VMEM((mats,) + block, BF16),
            pltpu.VMEM((n_slots,) + block, BF16),
            pltpu.VMEM((n_slots,) + block, BF16),
        ] + sems,
        compiler_params=pltpu.CompilerParams(collective_id=0, has_side_effects=True),
    )(slot_matrix, grads[0], momentum)
    return updates, renewed


def solution(mesh):
    return jax.shard_map(
        functools.partial(local, mesh.shape["dp"], mesh.shape["owner"]),
        mesh=mesh,
        in_specs=(P("dp", None, "owner", None), P("dp", "owner", None), P()),
        out_specs=(P(None, "owner", None), P("dp", "owner", None)),
        check_vma=False,
    )
```
